32 devices in a mesh: gy: 16 (over z, y, core), gz: 2 (over x).
Axes of the slice: x: 2, y: 2, z: 4, core: 2. Of those that a mesh axis runs over, the one named last changes fastest.
Arguments:
- random_fields: bfloat16 [16, 3, 2048, 512], P(None, None, 'gy', 'gz'), may hold values from -6 to 6
- previous: float32 [3, 2048, 512], P(None, 'gy', 'gz'), may hold values from -6 to 6
- decay: float32 [3, 512], P(None, 'gz'), may hold values from 0.2 to 0.95
- mean_flow: float32 [3, 512], P(None, 'gz'), may hold values from 0 to 1.5
- lund_diag: float32 [3, 512], P(None, 'gz'), may hold values from 0.3 to 1.5
- lund_off: float32 [3, 512], P(None, 'gz'), may hold values from -0.6 to 0.6
Outputs:
- velocity: float32 [16, 3, 2048, 512], P(None, None, 'gy', 'gz')
The draws below stay inside these ranges and needn't reach their ends.
All inputs are finite; a program needn't handle non-finite values.
Results may differ from the reference program's by a relative error of at most 0.0015.
The reference program's roundings to bfloat16 on the way count: a program that leaves them out, or rounds other values in their place, can miss the bound.
Values may be sent and summed in bfloat16 or wider, within the bound.
No kernel may reach another device: no remote copies, remote signals or barrier semaphores. Data moves between devices by JAX's collectives and lax.ppermute only.
A program may use at most 128 MiB of HBM per device.

```python
import math
import jax
import jax.numpy as jnp
from jax import lax

CY = 128
CZ = 256
STEPS = 16
HALF = 96
NY = 2048
NZ = 512


def draw_random_fields(key, part):
    values = jnp.clip(jax.random.normal(jax.random.fold_in(key, 303), (STEPS, 3, NY, NZ), jnp.float32), -6.0, 6.0)
    return values.astype(jnp.bfloat16)


def draw_previous(key, part):
    values = jnp.clip(jax.random.normal(jax.random.fold_in(key, 404), (3, NY, NZ), jnp.float32), -6.0, 6.0)
    return values


def draw_mean_flow(key, part):
    values = jax.random.uniform(jax.random.fold_in(key, 606), (3, NZ), jnp.float32, 0.0, 1.5)
    return values


def block_scale(key, shape, shards, low, largest):
    factor_of = 1.0
    for position, shards_of in shards:
        steps = jax.random.uniform(jax.random.fold_in(jax.random.fold_in(key, 6), position), (shards_of,), jnp.float32, low / len(shards), largest / len(shards))
        factor_of = factor_of * jnp.repeat(jnp.exp(steps), shape[position] // shards_of).reshape((-1,) + (1,) * (len(shape) - 1 - position))
    return factor_of


def setup_inputs(seed: int = 0) -> dict:
    arg_keys = jax.random.split(jax.random.key(seed), 7)
    return {
        "random_fields": draw_random_fields(jax.random.fold_in(arg_keys[6], 71), 0),
        "previous": draw_previous(jax.random.fold_in(arg_keys[6], 71), 0),
        "decay": jnp.clip(jnp.exp(math.log(0.95) - 1.5581446 * jax.random.uniform(arg_keys[2], (3, NZ), jnp.float32) ** block_scale(arg_keys[2], (3, NZ), ((1, 2),), -0.2, 0.2)), 0.2, 0.95),
        "mean_flow": draw_mean_flow(jax.random.fold_in(arg_keys[6], 71), 0),
        "lund_diag": jnp.clip(jnp.exp(math.log(1.5) - 1.60943787 * jax.random.uniform(arg_keys[4], (3, NZ), jnp.float32) ** block_scale(arg_keys[4], (3, NZ), ((1, 2),), -0.2, 0.2)), 0.3, 1.5),
        "lund_off": jnp.clip(jax.random.uniform(arg_keys[5], (3, NZ), jnp.float32, -0.6, 0.6) * block_scale(arg_keys[5], (3, NZ), ((1, 2),), -0.4, 0.0), -0.6, 0.6),
    }


def banded(rows):
    offsets = jnp.arange(-HALF, HALF + 1).astype(jnp.float32)
    scale = HALF * 1.0
    kernel = jnp.exp(-math.pi * offsets * offsets / (2.0 * scale * scale))
    norm = jnp.sqrt(jnp.sum(kernel * kernel))
    row_index = jnp.arange(rows).astype(jnp.int32)[:, None]
    col_index = jnp.arange(rows + 2 * HALF).astype(jnp.int32)[None, :]
    lag = (col_index - row_index - HALF).astype(jnp.float32)
    inside = jnp.abs(lag) <= HALF
    value = jnp.exp(-math.pi * lag * lag / (2.0 * scale * scale)) / norm
    return jnp.where(inside, value, jnp.zeros_like(value)).astype(jnp.bfloat16)

def filter_last(field, block, wrap):
    length = field.shape[-1]
    if wrap:
        padded = jnp.concatenate([field[..., length - HALF:], field, field[..., :HALF]], axis=-1)
    else:
        widths = [(0, 0)] * (field.ndim - 1) + [(HALF, HALF)]
        padded = jnp.pad(field, widths)
    matrix = banded(block).astype(jnp.float32)

    def one_block(start):
        piece = lax.dynamic_slice_in_dim(padded, start, block + 2 * HALF, padded.ndim - 1)
        return jnp.dot(piece, matrix.T, precision=lax.Precision.HIGHEST)
    starts = jnp.arange(length // block).astype(jnp.int32) * block
    blocks = lax.map(one_block, starts)
    return jnp.moveaxis(blocks, 0, -2).reshape(field.shape)

def lund_apply(state, mean_flow, lund_diag, lund_off):
    mean = mean_flow[:, None, :]
    diag = lund_diag[:, None, :]
    off = lund_off[:, None, :]
    first = mean[0] + diag[0] * state[0]
    second = mean[1] + off[0] * state[0] + diag[1] * state[1]
    third = mean[2] + off[1] * state[0] + off[2] * state[1] + diag[2] * state[2]
    return jnp.stack([first, second, third])

def reference(random_fields, previous, decay, mean_flow, lund_diag, lund_off):
    keep = decay[:, None, :]
    fresh = jnp.sqrt(1.0 - decay * decay)[:, None, :]

    def advance(state, raw):
        field = raw.astype(jnp.float32)
        along_span = filter_last(jnp.swapaxes(field, 1, 2), CY, True)
        rounded = lax.optimization_barrier(jnp.swapaxes(along_span, 1, 2).astype(jnp.bfloat16))
        filtered = filter_last(rounded.astype(jnp.float32), CZ, False)
        state = keep * state + fresh * filtered
        return (state, lund_apply(state, mean_flow, lund_diag, lund_off))
    final_state, velocity = lax.scan(advance, previous, random_fields)
    return velocity
```

```python
import functools
import math

import jax
import jax.numpy as jnp
from jax import lax
from jax.experimental import pallas as pl
from jax.experimental.pallas import tpu as pltpu
from jax.sharding import PartitionSpec as P

HALF = 96


def taps(lag):
    offsets = jnp.arange(-HALF, HALF + 1).astype(jnp.float32)
    scale = HALF * 1.0
    kernel = jnp.exp(-math.pi * offsets * offsets / (2.0 * scale * scale))
    norm = jnp.sqrt(jnp.sum(kernel * kernel))
    lag = lag.astype(jnp.float32)
    value = jnp.exp(-math.pi * lag * lag / (2.0 * scale * scale)) / norm
    return jnp.where(jnp.abs(lag) <= HALF, value, jnp.zeros_like(value)).astype(jnp.bfloat16)


def pairs(count, first, closed):
    found = []
    for low in range(first, count, 2):
        if low + 1 < count or closed:
            high = (low + 1) % count
            found += [(low, high), (high, low)]
    return found


def span_product(weights, core, own, link):
    planes = [jnp.concatenate([core[p], own[p], link[p]], axis=0) for p in range(len(own))]
    return jnp.dot(weights, jnp.concatenate(planes, axis=1), preferred_element_type=jnp.float32)


def smooth_far(block, start, first, count, where, weights, own, core, link):
    parts, lanes = own.shape[1], core.shape[3]
    lane = pl.multiple_of(where[block] * lanes, lanes)
    index = [(t, c) for t in range(count) for c in range(parts)]
    product = span_product(
        weights[...],
        [core[start + first + t, c] for t, c in index],
        [own[start + first + t, c, :, pl.ds(lane, lanes)] for t, c in index],
        [link[first + t, c] for t, c in index],
    ).astype(own.dtype)
    return {i: product[:, p * lanes : (p + 1) * lanes] for p, i in enumerate(index)}


def pack_kernel(chunks, where, fields, *refs):
    outs, sems = refs[:-1], refs[-1]
    copies = []
    for k, (start, count, side, block) in enumerate(chunks):
        rows, lanes = outs[k].shape[2:]
        row = pl.multiple_of(where[2 + side] * (fields.shape[2] - rows), math.gcd(fields.shape[2] - rows, 128))
        lane = pl.multiple_of(where[block] * lanes, lanes)
        copies.append(
            pltpu.make_async_copy(
                fields.at[pl.ds(start, count), :, pl.ds(row, rows), pl.ds(lane, lanes)], outs[k], sems.at[k]
            )
        )
    for copy in copies:
        copy.start()
    for copy in copies:
        copy.wait()


def smooth_kernel(start, block, per, where, weights, own, core, link, out, edge):
    steps = out.shape[0]
    width = edge.shape[2]
    for first in range(0, steps, per):
        planes = smooth_far(block, start, first, min(per, steps - first), where, weights, own, core, link)
        for (t, c), plane in planes.items():
            out[first + t, c] = plane
            turned = plane.T

            @pl.when(where[block] == 1)
            def _():
                edge[first + t, c] = turned[turned.shape[0] - width :, :]

            @pl.when(where[block] == 0)
            def _():
                edge[first + t, c] = turned[:width, :]


def velocity_kernel(halos, raw, start, near_first, per, where, weights, walls, *refs):
    (decay, mean, diag, off, before, own, core, link, near), rest = refs[:9], refs[9:]
    beside = rest[:halos]
    velocity, state = rest[-2:]
    parts, rows = own.shape[1:3]

    @pl.when(pl.program_id(0) == 0)
    def _():
        state[...] = before[...]

    first = pl.program_id(0) * per
    if raw:
        far = smooth_far(1, start, first, per, where, weights, own, core, link)
    else:
        far = {(t, c): own[first + t, c] for t in range(per) for c in range(parts)}
    index = [(t, c) for t in range(per) for c in range(parts)]
    cells = []
    for t, c in index:
        at = near_first + first + t
        cells.append(jnp.concatenate([far[t, c], near[at, c]] + [halo(first + t, c) for halo in halo_readers(beside, near_first)], axis=1))
    filtered = jnp.dot(jnp.concatenate(cells, axis=0), walls[...], preferred_element_type=jnp.float32)
    keep = decay[...]
    fresh = jnp.sqrt(1.0 - keep * keep)
    line = lambda x, c: x[c : c + 1, :]
    u, d, o = mean[...], diag[...], off[...]
    now = [state[c] for c in range(parts)]
    for t in range(per):
        for c in range(parts):
            p = t * parts + c
            now[c] = line(keep, c) * now[c] + line(fresh, c) * filtered[p * rows : (p + 1) * rows]
        velocity[t, 0] = line(u, 0) + line(d, 0) * now[0]
        velocity[t, 1] = line(u, 1) + line(o, 0) * now[0] + line(d, 1) * now[1]
        velocity[t, 2] = line(u, 2) + line(o, 1) * now[0] + line(o, 2) * now[1] + line(d, 2) * now[2]
    for c in range(parts):
        state[c] = now[c]


def halo_readers(beside, near_first):
    offsets = [near_first, 0]
    return [lambda t, c, ref=ref, o=o: ref[o + t, c].T for ref, o in zip(beside, offsets)]


def shards(random_fields, previous, decay, mean_flow, lund_diag, lund_off):
    steps, parts, rows, cols = random_fields.shape
    lanes = cols // 2
    span_count = lax.axis_size("gy")
    wall_count = lax.axis_size("gz")
    odd = lax.axis_index("gy") % 2
    wall_odd = lax.axis_index("gz") % 2
    near_block = 1 - wall_odd
    far_block = wall_odd
    where = jnp.stack([near_block, far_block, odd, 1 - odd]).astype(jnp.int32)

    core_pairs = pairs(span_count, 0, True)
    link_pairs = pairs(span_count, 1, True)
    near_pairs = pairs(wall_count, 0, False)
    far_pairs = pairs(wall_count, 1, False)

    half = steps // 2
    near_chunks = [(0, half), (half, steps - half)]
    last = max(1, steps // 4)
    far_chunks = [(0, half), (half, steps - half - last), (steps - last, last)]

    whole = pl.BlockSpec(memory_space=pltpu.VMEM)

    def pack(chunks):
        return pl.pallas_call(
            functools.partial(pack_kernel, chunks),
            out_shape=[jax.ShapeDtypeStruct((n, parts, HALF, lanes), random_fields.dtype) for _, n, _, _ in chunks],
            in_specs=[pl.BlockSpec(memory_space=pltpu.SMEM), pl.BlockSpec(memory_space=pltpu.HBM)],
            out_specs=[whole] * len(chunks),
            scratch_shapes=[pltpu.SemaphoreType.DMA((len(chunks),))],
            compiler_params=pltpu.CompilerParams(vmem_limit_bytes=16 * 2**20),
            cost_estimate=pl.CostEstimate(
                flops=0, bytes_accessed=4 * sum(n for _, n, _, _ in chunks) * parts * HALF * lanes, transcendentals=0
            ),
            name="pack",
        )(where, random_fields)

    cuts = [(s, n, 0, 0) for s, n in near_chunks] + [(0, steps, 1, 0)]
    cuts += [(s, n, 0, 1) for s, n in far_chunks] + [(0, steps, 1, 1)]
    (first_cut,) = pack(cuts[:1])
    received = [lax.ppermute(first_cut, "gy", link_pairs)]
    for cut, x in zip(cuts[1:], pack(cuts[1:])):
        received.append(lax.ppermute(x, "gy", core_pairs if cut[2] else link_pairs))
    near_link, near_core = received[: len(near_chunks)], received[len(near_chunks)]
    far_link, far_core = received[len(near_chunks) + 1 : -1], received[-1]

    i = jnp.arange(rows)[:, None]
    j = jnp.arange(HALF)[None, :]
    left, right = j - HALF - i, rows + j - i
    weights = taps(
        jnp.concatenate(
            [jnp.where(odd == 1, left, right), jnp.arange(rows)[None, :] - i, jnp.where(odd == 1, right, left)], axis=1
        )
    )
    m = jnp.arange(cols)[None, :]
    j = jnp.arange(lanes)[:, None]
    h = jnp.arange(HALF)[:, None]
    before_block, after_block = h - HALF - m, cols + h - m
    columns = [far_block * lanes + j - m, near_block * lanes + j - m]
    if near_pairs:
        columns.append(jnp.where(wall_odd == 1, before_block, after_block))
    if far_pairs:
        columns.append(jnp.where(wall_odd == 1, after_block, before_block))
    walls = taps(jnp.concatenate(columns, axis=0))

    def smooth(start, count, block, core, link):
        return pl.pallas_call(
            functools.partial(smooth_kernel, start, block, 4),
            out_shape=(
                jax.ShapeDtypeStruct((count, parts, rows, lanes), jnp.bfloat16),
                jax.ShapeDtypeStruct((count, parts, HALF, rows), jnp.bfloat16),
            ),
            in_specs=[pl.BlockSpec(memory_space=pltpu.SMEM)] + [whole] * 4,
            out_specs=(whole, whole),
            compiler_params=pltpu.CompilerParams(vmem_limit_bytes=24 * 2**20),
            cost_estimate=pl.CostEstimate(
                flops=2 * count * parts * rows * lanes * (rows + 2 * HALF),
                bytes_accessed=4 * count * parts * lanes * (rows + HALF),
                transcendentals=0,
            ),
            name="smooth",
        )(where, weights, random_fields, core, link)

    near = [smooth(s, n, 0, near_core, link) for (s, n), link in zip(near_chunks, near_link)]
    near_halo = [lax.ppermute(edge, "gz", near_pairs) for _, edge in near] if near_pairs else []
    far, far_halo = None, []
    if far_pairs:
        far = [smooth(s, n, 1, far_core, link) for (s, n), link in zip(far_chunks, far_link)]
        far_halo = [lax.ppermute(edge, "gz", far_pairs) for _, edge in far]

    velocity, state = None, previous
    for k, (s, n) in enumerate(far_chunks):
        source = max(q for q, (start, _) in enumerate(near_chunks) if start <= s)
        per = math.gcd(math.gcd(n, s), 2)
        operands = [where, weights, walls, decay, mean_flow, lund_diag, lund_off, state]
        operands += [random_fields if far is None else far[k][0], far_core, far_link[k], near[source][0]]
        beside = near_halo[source : source + 1] + far_halo[k : k + 1]
        operands += beside
        specs = [pl.BlockSpec(memory_space=pltpu.SMEM)] + [whole] * (len(operands) - 1)
        aliases = {}
        if velocity is not None:
            aliases = {len(operands): 0}
            operands.append(velocity)
            specs.append(pl.BlockSpec(memory_space=pl.ANY))
        velocity, state = pl.pallas_call(
            functools.partial(
                velocity_kernel, len(beside), far is None, s, s - near_chunks[source][0], per
            ),
            out_shape=(
                jax.ShapeDtypeStruct((steps, parts, rows, cols), jnp.float32),
                jax.ShapeDtypeStruct(previous.shape, jnp.float32),
            ),
            grid=(n // per,),
            in_specs=specs,
            out_specs=(
                pl.BlockSpec((per, parts, rows, cols), functools.partial(lambda o, t: (o + t, 0, 0, 0), s // per)),
                whole,
            ),
            input_output_aliases=aliases,
            compiler_params=pltpu.CompilerParams(vmem_limit_bytes=24 * 2**20),
            cost_estimate=pl.CostEstimate(
                flops=2 * n * parts * rows * (lanes * (rows + 2 * HALF) + cols * walls.shape[0]),
                bytes_accessed=n * parts * rows * (4 * cols + 10 * lanes),
                transcendentals=0,
            ),
            name="velocity",
        )(*operands)
    return velocity


def solution(mesh):
    return jax.shard_map(
        shards,
        mesh=mesh,
        in_specs=(
            P(None, None, "gy", "gz"),
            P(None, "gy", "gz"),
            P(None, "gz"),
            P(None, "gz"),
            P(None, "gz"),
            P(None, "gz"),
        ),
        out_specs=P(None, None, "gy", "gz"),
        check_vma=False,
    )
```

```python
import functools
import math

import jax
import jax.numpy as jnp
from jax import lax
from jax.experimental import pallas as pl
from jax.experimental.pallas import tpu as pltpu
from jax.sharding import PartitionSpec as P

HALF = 96


def taps(lag):
    offsets = jnp.arange(-HALF, HALF + 1).astype(jnp.float32)
    scale = HALF * 1.0
    kernel = jnp.exp(-math.pi * offsets * offsets / (2.0 * scale * scale))
    norm = jnp.sqrt(jnp.sum(kernel * kernel))
    lag = lag.astype(jnp.float32)
    value = jnp.exp(-math.pi * lag * lag / (2.0 * scale * scale)) / norm
    return jnp.where(jnp.abs(lag) <= HALF, value, jnp.zeros_like(value)).astype(jnp.bfloat16)


def pairs(count, first, closed):
    found = []
    for low in range(first, count, 2):
        if low + 1 < count or closed:
            high = (low + 1) % count
            found += [(low, high), (high, low)]
    return found


def span_product(weights, core, own, link):
    planes = [jnp.concatenate([core[p], own[p], link[p]], axis=0) for p in range(len(own))]
    return jnp.dot(weights, jnp.concatenate(planes, axis=1), preferred_element_type=jnp.float32)


def smooth_far(block, start, first, count, where, weights, own, core, link):
    parts, lanes = own.shape[1], core.shape[3]
    lane = pl.multiple_of(where[block] * lanes, lanes)
    index = [(t, c) for t in range(count) for c in range(parts)]
    product = span_product(
        weights[...],
        [core[start + first + t, c] for t, c in index],
        [own[start + first + t, c, :, pl.ds(lane, lanes)] for t, c in index],
        [link[first + t, c] for t, c in index],
    ).astype(own.dtype)
    return {i: product[:, p * lanes : (p + 1) * lanes] for p, i in enumerate(index)}


def smooth_kernel(start, block, per, where, weights, own, core, link, out, edge):
    steps = out.shape[0]
    width = edge.shape[2]
    for first in range(0, steps, per):
        planes = smooth_far(block, start, first, min(per, steps - first), where, weights, own, core, link)
        for (t, c), plane in planes.items():
            out[first + t, c] = plane
            turned = plane.T

            @pl.when(where[block] == 1)
            def _():
                edge[first + t, c] = turned[turned.shape[0] - width :, :]

            @pl.when(where[block] == 0)
            def _():
                edge[first + t, c] = turned[:width, :]


def velocity_kernel(halos, raw, start, near_first, per, where, weights, walls, *refs):
    (decay, mean, diag, off, before, own, core, link, near), rest = refs[:9], refs[9:]
    beside = rest[:halos]
    velocity, state = rest[-2:]
    parts, rows = own.shape[1:3]

    @pl.when(pl.program_id(0) == 0)
    def _():
        state[...] = before[...]

    first = pl.program_id(0) * per
    if raw:
        far = smooth_far(1, start, first, per, where, weights, own, core, link)
    else:
        far = {(t, c): own[first + t, c] for t in range(per) for c in range(parts)}
    index = [(t, c) for t in range(per) for c in range(parts)]
    cells = []
    for t, c in index:
        at = near_first + first + t
        cells.append(jnp.concatenate([far[t, c], near[at, c]] + [halo(first + t, c) for halo in halo_readers(beside, near_first)], axis=1))
    filtered = jnp.dot(jnp.concatenate(cells, axis=0), walls[...], preferred_element_type=jnp.float32)
    keep = decay[...]
    fresh = jnp.sqrt(1.0 - keep * keep)
    line = lambda x, c: x[c : c + 1, :]
    u, d, o = mean[...], diag[...], off[...]
    now = [state[c] for c in range(parts)]
    for t in range(per):
        for c in range(parts):
            p = t * parts + c
            now[c] = line(keep, c) * now[c] + line(fresh, c) * filtered[p * rows : (p + 1) * rows]
        velocity[t, 0] = line(u, 0) + line(d, 0) * now[0]
        velocity[t, 1] = line(u, 1) + line(o, 0) * now[0] + line(d, 1) * now[1]
        velocity[t, 2] = line(u, 2) + line(o, 1) * now[0] + line(o, 2) * now[1] + line(d, 2) * now[2]
    for c in range(parts):
        state[c] = now[c]


def halo_readers(beside, near_first):
    offsets = [near_first, 0]
    return [lambda t, c, ref=ref, o=o: ref[o + t, c].T for ref, o in zip(beside, offsets)]


def chunks_of(steps):
    half, last = steps // 2, max(1, steps // 4)
    return [(0, half), (half, steps - half)], [(0, half), (half, steps - half - last), (steps - last, last)]


def shards(random_fields, previous, decay, mean_flow, lund_diag, lund_off):
    steps, parts, rows, cols = random_fields.shape
    lanes = cols // 2
    span_count = lax.axis_size("gy")
    wall_count = lax.axis_size("gz")
    odd = lax.axis_index("gy") % 2
    wall_odd = lax.axis_index("gz") % 2
    near_block = 1 - wall_odd
    far_block = wall_odd
    where = jnp.stack([near_block, far_block]).astype(jnp.int32)

    core_pairs = pairs(span_count, 0, True)
    link_pairs = pairs(span_count, 1, True)
    near_pairs = pairs(wall_count, 0, False)
    far_pairs = pairs(wall_count, 1, False)

    near_chunks, far_chunks = chunks_of(steps)
    whole = pl.BlockSpec(memory_space=pltpu.VMEM)

    link_row, core_row = odd * (rows - HALF), (1 - odd) * (rows - HALF)

    def cut(fields, start, count, row, block):
        return lax.dynamic_slice(fields, (start, 0, row, block * lanes), (count, parts, HALF, lanes))

    first_cut = cut(random_fields, *near_chunks[0], link_row, near_block)
    fields, first_cut = lax.optimization_barrier((random_fields, first_cut))
    near_cuts = [first_cut] + [cut(fields, s, n, link_row, near_block) for s, n in near_chunks[1:]]
    far_cuts = [cut(fields, s, n, link_row, far_block) for s, n in far_chunks]
    near_core = lax.ppermute(cut(fields, 0, steps, core_row, near_block), "gy", core_pairs)
    far_core = lax.ppermute(cut(fields, 0, steps, core_row, far_block), "gy", core_pairs)
    links = [lax.ppermute(x, "gy", link_pairs) for x in near_cuts + far_cuts]
    near_link, far_link = links[: len(near_chunks)], links[len(near_chunks) :]

    i = jnp.arange(rows)[:, None]
    j = jnp.arange(HALF)[None, :]
    left, right = j - HALF - i, rows + j - i
    weights = taps(
        jnp.concatenate(
            [jnp.where(odd == 1, left, right), jnp.arange(rows)[None, :] - i, jnp.where(odd == 1, right, left)], axis=1
        )
    )
    m = jnp.arange(cols)[None, :]
    j = jnp.arange(lanes)[:, None]
    h = jnp.arange(HALF)[:, None]
    before_block, after_block = h - HALF - m, cols + h - m
    columns = [far_block * lanes + j - m, near_block * lanes + j - m]
    if near_pairs:
        columns.append(jnp.where(wall_odd == 1, before_block, after_block))
    if far_pairs:
        columns.append(jnp.where(wall_odd == 1, after_block, before_block))
    walls = taps(jnp.concatenate(columns, axis=0))
    weights, walls = lax.optimization_barrier((weights, walls))

    def smooth(start, count, block, core, link):
        return pl.pallas_call(
            functools.partial(smooth_kernel, start, block, 4),
            out_shape=(
                jax.ShapeDtypeStruct((count, parts, rows, lanes), jnp.bfloat16),
                jax.ShapeDtypeStruct((count, parts, HALF, rows), jnp.bfloat16),
            ),
            in_specs=[pl.BlockSpec(memory_space=pltpu.SMEM)] + [whole] * 4,
            out_specs=(whole, whole),
            compiler_params=pltpu.CompilerParams(vmem_limit_bytes=12 * 2**20),
            cost_estimate=pl.CostEstimate(
                flops=2 * count * parts * rows * lanes * (rows + 2 * HALF),
                bytes_accessed=4 * count * parts * lanes * (rows + HALF),
                transcendentals=0,
            ),
            name="smooth",
        )(where, weights, random_fields, core, link)

    near = [smooth(s, n, 0, near_core, link) for (s, n), link in zip(near_chunks, near_link)]
    near_halo = []
    if near_pairs:
        near_halo = [lax.ppermute(edge, "gz", near_pairs) for _, edge in near]
    far, far_halo = None, []
    if far_pairs:
        far = [smooth(s, n, 1, far_core, link) for (s, n), link in zip(far_chunks, far_link)]
        far_halo = [lax.ppermute(edge, "gz", far_pairs) for _, edge in far]

    velocity, state = None, previous
    for k, (s, n) in enumerate(far_chunks):
        source = max(q for q, (start, _) in enumerate(near_chunks) if start <= s)
        per = math.gcd(math.gcd(n, s), 2)
        operands = [where, weights, walls, decay, mean_flow, lund_diag, lund_off, state]
        operands += [random_fields if far is None else far[k][0], far_core, far_link[k], near[source][0]]
        beside = near_halo[source : source + 1] + far_halo[k : k + 1]
        operands += beside
        specs = [pl.BlockSpec(memory_space=pltpu.SMEM)] + [whole] * (len(operands) - 1)
        aliases = {}
        if velocity is not None:
            aliases = {len(operands): 0}
            operands.append(velocity)
            specs.append(pl.BlockSpec(memory_space=pl.ANY))
        velocity, state = pl.pallas_call(
            functools.partial(
                velocity_kernel, len(beside), far is None, s, s - near_chunks[source][0], per
            ),
            out_shape=(
                jax.ShapeDtypeStruct((steps, parts, rows, cols), jnp.float32),
                jax.ShapeDtypeStruct(previous.shape, jnp.float32),
            ),
            grid=(n // per,),
            in_specs=specs,
            out_specs=(
                pl.BlockSpec((per, parts, rows, cols), functools.partial(lambda o, t: (o + t, 0, 0, 0), s // per)),
                whole,
            ),
            input_output_aliases=aliases,
            compiler_params=pltpu.CompilerParams(vmem_limit_bytes=12 * 2**20),
            cost_estimate=pl.CostEstimate(
                flops=2 * n * parts * rows * (lanes * (rows + 2 * HALF) + cols * walls.shape[0]),
                bytes_accessed=n * parts * rows * (4 * cols + 10 * lanes),
                transcendentals=0,
            ),
            name="velocity",
        )(*operands)
    return velocity


def solution(mesh):
    return jax.shard_map(
        shards,
        mesh=mesh,
        in_specs=(
            P(None, None, "gy", "gz"),
            P(None, "gy", "gz"),
            P(None, "gz"),
            P(None, "gz"),
            P(None, "gz"),
            P(None, "gz"),
        ),
        out_specs=P(None, None, "gy", "gz"),
        check_vma=False,
    )
```

```python
import functools
import math

import jax
import jax.numpy as jnp
from jax import lax
from jax.experimental import pallas as pl
from jax.experimental.pallas import tpu as pltpu
from jax.sharding import PartitionSpec as P

HALF = 96


VMEM = pl.BlockSpec(memory_space=pltpu.VMEM)
GRANT = 12 * 2**20


def pairs(count, first, closed):
    found = []
    for low in range(first, count, 2):
        if low + 1 < count or closed:
            high = (low + 1) % count
            found += [(low, high), (high, low)]
    return found


def chunks_of(steps):
    ends = [max(1, steps // 4), max(1, (5 * steps) // 8), steps]
    near = [(a, b - a) for a, b in zip([0] + ends, ends) if b > a]
    start, count = near[-1]
    last = count // 3
    far = near[:-1] + ([(start, count - last), (start + count - last, last)] if last else near[-1:])
    return near, far


def parity(axis):
    return lax.axis_index(axis) % 2


def half_of(block):
    odd = parity("gz")
    return odd if block else 1 - odd


def taps(lag):
    scale = HALF * 1.0
    offsets = lax.broadcasted_iota(jnp.int32, (8, 2 * HALF + 1), 1) - HALF
    offsets = offsets.astype(jnp.float32)
    kernel = jnp.exp(-math.pi * offsets * offsets / (2.0 * scale * scale))
    norm = jnp.sqrt(jnp.sum(kernel * kernel, axis=1, keepdims=True))[:1, :1]
    lag = lag.astype(jnp.float32)
    value = jnp.exp(-math.pi * lag * lag / (2.0 * scale * scale)) / norm
    return jnp.where(jnp.abs(lag) <= HALF, value, jnp.zeros_like(value)).astype(jnp.bfloat16)


def bands_kernel(weights, walls):
    rows = weights.shape[0]
    before, after = -HALF, rows
    odd = parity("gy")
    i = lax.broadcasted_iota(jnp.int32, weights.shape, 0)
    j = lax.broadcasted_iota(jnp.int32, weights.shape, 1)
    at_core = j + jnp.where(odd == 1, before, after)
    at_link = j - HALF - rows + jnp.where(odd == 1, after, before)
    at = jnp.where(j < HALF, at_core, jnp.where(j < HALF + rows, j - HALF, at_link))
    weights[...] = taps(at - i)

    cols = walls.shape[1]
    lanes = cols // 2
    odd = parity("gz")
    j = lax.broadcasted_iota(jnp.int32, walls.shape, 0)
    m = lax.broadcasted_iota(jnp.int32, walls.shape, 1)
    at_far = j + half_of(1) * lanes
    at_near = j - lanes + half_of(0) * lanes
    at_near_halo = j - cols + jnp.where(odd == 1, -HALF, cols)
    at_far_halo = j - cols - HALF + jnp.where(odd == 1, cols, -HALF)
    at = jnp.where(j < cols + HALF, at_near_halo, at_far_halo)
    at = jnp.where(j < lanes, at_far, jnp.where(j < cols, at_near, at))
    walls[...] = taps(at - m)


def pack_kernel(cuts, own, *outs):
    rows = own.shape[2]
    for (start, count, side, block), out in zip(cuts, outs):
        lanes = out.shape[3]
        odd = parity("gy")
        row = pl.multiple_of((1 - odd if side else odd) * (rows - HALF), math.gcd(rows - HALF, 128))
        lane = pl.multiple_of(half_of(block) * lanes, lanes)
        for t in range(count):
            for c in range(own.shape[1]):
                out[t, c] = own[start + t, c, pl.ds(row, HALF), pl.ds(lane, lanes)]


def span_product(weights, core, own, link):
    planes = [jnp.concatenate([core[p], own[p], link[p]], axis=0) for p in range(len(own))]
    return jnp.dot(weights, jnp.concatenate(planes, axis=1), preferred_element_type=jnp.float32)


def smooth_planes(block, start, first, count, weights, own, core, link):
    parts, lanes = own.shape[1], core.shape[3]
    lane = pl.multiple_of(half_of(block) * lanes, lanes)
    index = [(t, c) for t in range(count) for c in range(parts)]
    product = span_product(
        weights[...],
        [core[start + first + t, c] for t, c in index],
        [own[start + first + t, c, :, pl.ds(lane, lanes)] for t, c in index],
        [link[first + t, c] for t, c in index],
    ).astype(own.dtype)
    return {i: product[:, p * lanes : (p + 1) * lanes] for p, i in enumerate(index)}


def smooth_kernel(start, block, per, weights, own, core, link, out, edge):
    steps = out.shape[0]
    width = edge.shape[2]
    for first in range(0, steps, per):
        planes = smooth_planes(block, start, first, min(per, steps - first), weights, own, core, link)
        upper = half_of(block)
        for (t, c), plane in planes.items():
            out[first + t, c] = plane
        turned = {i: plane.T for i, plane in planes.items()}

        @pl.when(upper == 1)
        def _():
            for (t, c), plane in turned.items():
                edge[first + t, c] = plane[plane.shape[0] - width :, :]

        @pl.when(upper == 0)
        def _():
            for (t, c), plane in turned.items():
                edge[first + t, c] = plane[:width, :]


def velocity_kernel(halos, raw, start, near_first, per, weights, walls, *refs):
    (decay, mean, diag, off, before, own, core, link, near), rest = refs[:9], refs[9:]
    beside = rest[:halos]
    velocity, state = rest[-2:]
    parts, rows = own.shape[1:3]

    @pl.when(pl.program_id(0) == 0)
    def _():
        state[...] = before[...]

    first = pl.program_id(0) * per
    index = [(t, c) for t in range(per) for c in range(parts)]
    if raw:
        far = smooth_planes(1, start, first, per, weights, own, core, link)
    else:
        far = {(t, c): own[first + t, c] for t, c in index}
    offsets = [near_first, 0]
    cells = []
    for t, c in index:
        sides = [ref[offset + first + t, c].T for ref, offset in zip(beside, offsets)]
        cells.append(jnp.concatenate([far[t, c], near[near_first + first + t, c]] + sides, axis=1))
    filtered = jnp.dot(jnp.concatenate(cells, axis=0), walls[...], preferred_element_type=jnp.float32)
    keep = decay[...]
    fresh = jnp.sqrt(1.0 - keep * keep)
    line = lambda x, c: x[c : c + 1, :]
    u, d, o = mean[...], diag[...], off[...]
    now = [state[c] for c in range(parts)]
    for t in range(per):
        for c in range(parts):
            p = t * parts + c
            now[c] = line(keep, c) * now[c] + line(fresh, c) * filtered[p * rows : (p + 1) * rows]
        velocity[t, 0] = line(u, 0) + line(d, 0) * now[0]
        velocity[t, 1] = line(u, 1) + line(o, 0) * now[0] + line(d, 1) * now[1]
        velocity[t, 2] = line(u, 2) + line(o, 1) * now[0] + line(o, 2) * now[1] + line(d, 2) * now[2]
    for c in range(parts):
        state[c] = now[c]


def shards(random_fields, previous, decay, mean_flow, lund_diag, lund_off):
    steps, parts, rows, cols = random_fields.shape
    lanes = cols // 2
    span_count = lax.axis_size("gy")
    wall_count = lax.axis_size("gz")
    kind = random_fields.dtype
    params = pltpu.CompilerParams(vmem_limit_bytes=GRANT)

    core_pairs = pairs(span_count, 0, True)
    link_pairs = pairs(span_count, 1, True)
    near_pairs = pairs(wall_count, 0, False)
    far_pairs = pairs(wall_count, 1, False)
    near_chunks, far_chunks = chunks_of(steps)

    start, count = near_chunks[0]
    first_cut = lax.dynamic_slice(
        random_fields,
        (start, 0, parity("gy") * (rows - HALF), half_of(0) * lanes),
        (count, parts, HALF, lanes),
    )
    own, first_cut = lax.optimization_barrier((random_fields, first_cut))

    cuts = [(0, steps, 1, 0)] + [(s, n, 0, 0) for s, n in near_chunks[1:]]
    cuts += [(s, n, 0, 1) for s, n in far_chunks] + [(0, steps, 1, 1)]
    packed = pl.pallas_call(
        functools.partial(pack_kernel, cuts),
        out_shape=[jax.ShapeDtypeStruct((n, parts, HALF, lanes), kind) for _, n, _, _ in cuts],
        in_specs=[VMEM],
        out_specs=[VMEM] * len(cuts),
        compiler_params=params,
        name="pack",
    )(own)
    near_core = lax.ppermute(packed[0], "gy", core_pairs)
    far_core = lax.ppermute(packed[-1], "gy", core_pairs)
    links = [lax.ppermute(x, "gy", link_pairs) for x in [first_cut, *packed[1:-1]]]
    near_link, far_link = links[: len(near_chunks)], links[len(near_chunks) :]

    depth = cols + HALF * (bool(near_pairs) + bool(far_pairs))
    weights, walls = pl.pallas_call(
        bands_kernel,
        out_shape=(
            jax.ShapeDtypeStruct((rows, rows + 2 * HALF), kind),
            jax.ShapeDtypeStruct((depth, cols), kind),
        ),
        out_specs=(VMEM, VMEM),
        compiler_params=params,
        name="bands",
    )()

    def smooth(start, count, block, core, link):
        return pl.pallas_call(
            functools.partial(smooth_kernel, start, block, 3),
            out_shape=(
                jax.ShapeDtypeStruct((count, parts, rows, lanes), kind),
                jax.ShapeDtypeStruct((count, parts, HALF, rows), kind),
            ),
            in_specs=[VMEM] * 4,
            out_specs=(VMEM, VMEM),
            compiler_params=params,
            cost_estimate=pl.CostEstimate(
                flops=2 * count * parts * rows * lanes * (rows + 2 * HALF),
                bytes_accessed=4 * count * parts * lanes * (rows + HALF),
                transcendentals=0,
            ),
            name="smooth",
        )(weights, own, core, link)

    near = [smooth(s, n, 0, near_core, link) for (s, n), link in zip(near_chunks, near_link)]
    near_halo, far_halo, far = [], [], None
    if near_pairs:
        near_halo = [lax.ppermute(edge, "gz", near_pairs) for _, edge in near]
    if far_pairs:
        far = [smooth(s, n, 1, far_core, link) for (s, n), link in zip(far_chunks, far_link)]
        far_halo = [lax.ppermute(edge, "gz", far_pairs) for _, edge in far]

    velocity, state = None, previous
    for k, (s, n) in enumerate(far_chunks):
        source = max(q for q, (first, _) in enumerate(near_chunks) if first <= s)
        per = math.gcd(math.gcd(n, s), 2)
        operands = [weights, walls, decay, mean_flow, lund_diag, lund_off, state]
        operands += [own if far is None else far[k][0], far_core, far_link[k], near[source][0]]
        beside = near_halo[source : source + 1] + far_halo[k : k + 1]
        operands += beside
        specs = [VMEM] * len(operands)
        aliases = {}
        if velocity is not None:
            aliases = {len(operands): 0}
            operands.append(velocity)
            specs.append(pl.BlockSpec(memory_space=pl.ANY))
        velocity, state = pl.pallas_call(
            functools.partial(velocity_kernel, len(beside), far is None, s, s - near_chunks[source][0], per),
            out_shape=(
                jax.ShapeDtypeStruct((steps, parts, rows, cols), jnp.float32),
                jax.ShapeDtypeStruct(previous.shape, jnp.float32),
            ),
            grid=(n // per,),
            in_specs=specs,
            out_specs=(
                pl.BlockSpec((per, parts, rows, cols), functools.partial(lambda o, t: (o + t, 0, 0, 0), s // per)),
                VMEM,
            ),
            input_output_aliases=aliases,
            compiler_params=params,
            cost_estimate=pl.CostEstimate(
                flops=2 * n * parts * rows * (lanes * (rows + 2 * HALF) + cols * depth),
                bytes_accessed=n * parts * rows * (4 * cols + 10 * lanes),
                transcendentals=0,
            ),
            name="velocity",
        )(*operands)
    return velocity


def solution(mesh):
    return jax.shard_map(
        shards,
        mesh=mesh,
        in_specs=(
            P(None, None, "gy", "gz"),
            P(None, "gy", "gz"),
            P(None, "gz"),
            P(None, "gz"),
            P(None, "gz"),
            P(None, "gz"),
        ),
        out_specs=P(None, None, "gy", "gz"),
        check_vma=False,
    )
```

```python
import functools
import math

import jax
import jax.numpy as jnp
from jax import lax
from jax.experimental import pallas as pl
from jax.experimental.pallas import tpu as pltpu
from jax.sharding import PartitionSpec as P

HALF = 96


VMEM = pl.BlockSpec(memory_space=pltpu.VMEM)
GRANT = 12 * 2**20


def pairs(count, first, closed):
    found = []
    for low in range(first, count, 2):
        if low + 1 < count or closed:
            high = (low + 1) % count
            found += [(low, high), (high, low)]
    return found


def chunks_of(steps):
    cut = lambda ends: [(a, b - a) for a, b in zip([0] + ends, ends)]
    sixteenths = lambda *parts: sorted({max(1, p * steps // 16) for p in parts})
    return cut(sixteenths(3, 8, 12, 16)), cut(sorted({*sixteenths(8, 12, 16), max(1, steps - 1)}))


def parity(axis):
    return lax.axis_index(axis) % 2


def half_of(block):
    odd = parity("gz")
    return odd if block else 1 - odd


def taps(lag):
    scale = HALF * 1.0
    offsets = lax.broadcasted_iota(jnp.int32, (8, 2 * HALF + 1), 1) - HALF
    offsets = offsets.astype(jnp.float32)
    kernel = jnp.exp(-math.pi * offsets * offsets / (2.0 * scale * scale))
    norm = jnp.sqrt(jnp.sum(kernel * kernel, axis=1, keepdims=True))[:1, :1]
    lag = lag.astype(jnp.float32)
    value = jnp.exp(-math.pi * lag * lag / (2.0 * scale * scale)) / norm
    return jnp.where(jnp.abs(lag) <= HALF, value, jnp.zeros_like(value)).astype(jnp.bfloat16)


def bands_kernel(weights, walls):
    rows = weights.shape[0]
    before, after = -HALF, rows
    odd = parity("gy")
    i = lax.broadcasted_iota(jnp.int32, weights.shape, 0)
    j = lax.broadcasted_iota(jnp.int32, weights.shape, 1)
    at_core = j + jnp.where(odd == 1, before, after)
    at_link = j - HALF - rows + jnp.where(odd == 1, after, before)
    at = jnp.where(j < HALF, at_core, jnp.where(j < HALF + rows, j - HALF, at_link))
    weights[...] = taps(at - i)

    cols = walls.shape[1]
    lanes = cols // 2
    odd = parity("gz")
    j = lax.broadcasted_iota(jnp.int32, walls.shape, 0)
    m = lax.broadcasted_iota(jnp.int32, walls.shape, 1)
    at_far = j + half_of(1) * lanes
    at_near = j - lanes + half_of(0) * lanes
    at_near_halo = j - cols + jnp.where(odd == 1, -HALF, cols)
    at_far_halo = j - cols - HALF + jnp.where(odd == 1, cols, -HALF)
    at = jnp.where(j < cols + HALF, at_near_halo, at_far_halo)
    at = jnp.where(j < lanes, at_far, jnp.where(j < cols, at_near, at))
    walls[...] = taps(at - m)


def pack_kernel(cuts, own, *outs):
    rows = own.shape[2]
    for (start, count, side, block), out in zip(cuts, outs):
        lanes = out.shape[3]
        odd = parity("gy")
        row = pl.multiple_of((1 - odd if side else odd) * (rows - HALF), math.gcd(rows - HALF, 128))
        lane = pl.multiple_of(half_of(block) * lanes, lanes)
        for t in range(count):
            for c in range(own.shape[1]):
                out[t, c] = own[start + t, c, pl.ds(row, HALF), pl.ds(lane, lanes)]


def span_product(weights, core, own, link):
    planes = [jnp.concatenate([core[p], own[p], link[p]], axis=0) for p in range(len(own))]
    return jnp.dot(weights, jnp.concatenate(planes, axis=1), preferred_element_type=jnp.float32)


def smooth_planes(block, start, first, count, weights, own, core, link):
    parts, lanes = own.shape[1], core.shape[3]
    lane = pl.multiple_of(half_of(block) * lanes, lanes)
    index = [(t, c) for t in range(count) for c in range(parts)]
    product = span_product(
        weights[...],
        [core[start + first + t, c] for t, c in index],
        [own[start + first + t, c, :, pl.ds(lane, lanes)] for t, c in index],
        [link[first + t, c] for t, c in index],
    ).astype(own.dtype)
    return {i: product[:, p * lanes : (p + 1) * lanes] for p, i in enumerate(index)}


def smooth_kernel(start, block, per, weights, own, core, link, out, edge):
    steps = out.shape[0]
    width = edge.shape[2]
    for first in range(0, steps, per):
        planes = smooth_planes(block, start, first, min(per, steps - first), weights, own, core, link)
        upper = half_of(block)
        for (t, c), plane in planes.items():
            out[first + t, c] = plane
        turned = {i: plane.T for i, plane in planes.items()}

        @pl.when(upper == 1)
        def _():
            for (t, c), plane in turned.items():
                edge[first + t, c] = plane[plane.shape[0] - width :, :]

        @pl.when(upper == 0)
        def _():
            for (t, c), plane in turned.items():
                edge[first + t, c] = plane[:width, :]


def velocity_kernel(chunk, sources, raw, halos, kept, last, *refs):
    start, count = chunk
    (weights, walls, decay, mean, diag, off, before, own, core, link), rest = refs[:10], refs[10:]
    near, rest = rest[: len(sources)], rest[len(sources) :]
    near_halo, rest = (rest[: len(sources)], rest[len(sources) :]) if halos[0] else ((), rest)
    far_halo, rest = (rest[:1], rest[1:]) if halos[1] else ((), rest)
    kept_ref, rest = (rest[0], rest[1:]) if kept else (None, rest)
    if last:
        velocity, out, sems = rest[-3:]
    elif kept:
        velocity, state, out, sems = rest[-4:]
    else:
        state, out = rest
    copies = []
    if kept:
        copies.append(pltpu.make_async_copy(kept_ref, velocity.at[pl.ds(*kept)], sems.at[0]))
        copies[0].start()

    parts, rows = own.shape[1:3]
    keep = decay[...]
    fresh = jnp.sqrt(1.0 - keep * keep)
    line = lambda x, c: x[c : c + 1, :]
    u, d, o = mean[...], diag[...], off[...]
    band = walls[...]
    now = [before[c] for c in range(parts)]
    for first in range(0, count, 2):
        group = range(first, min(first + 2, count))
        if raw:
            far = smooth_planes(1, start, first, len(group), weights, own, core, link)
        for t in group:
            step = start + t
            q = max(q for q, at in enumerate(sources) if at <= step)
            cells = []
            for c in range(parts):
                row = [far[t - first, c] if raw else own[t, c], near[q][step - sources[q], c]]
                row += [ref[step - sources[q], c].T for ref in near_halo[q : q + 1]]
                row += [ref[t, c].T for ref in far_halo]
                cells.append(jnp.concatenate(row, axis=1))
            filtered = jnp.dot(jnp.concatenate(cells, axis=0), band, preferred_element_type=jnp.float32)
            for c in range(parts):
                now[c] = line(keep, c) * now[c] + line(fresh, c) * filtered[c * rows : (c + 1) * rows]
                value = line(u, c) + line(d, c) * now[c]
                for e in range(c):
                    value = value + line(o, (c * (c - 1)) // 2 + e) * now[e]
                out[t, c] = value
                if last:
                    k = bool(kept) + t * parts + c
                    copies.append(pltpu.make_async_copy(out.at[t, c], velocity.at[step, c], sems.at[k]))
                    copies[-1].start()
    if not last:
        for c in range(parts):
            state[c] = now[c]
    for copy in copies:
        copy.wait()


def shards(random_fields, previous, decay, mean_flow, lund_diag, lund_off):
    steps, parts, rows, cols = random_fields.shape
    lanes = cols // 2
    span_count = lax.axis_size("gy")
    wall_count = lax.axis_size("gz")
    kind = random_fields.dtype
    params = pltpu.CompilerParams(vmem_limit_bytes=GRANT)

    core_pairs = pairs(span_count, 0, True)
    link_pairs = pairs(span_count, 1, True)
    near_pairs = pairs(wall_count, 0, False)
    far_pairs = pairs(wall_count, 1, False)
    near_chunks, far_chunks = chunks_of(steps)

    start, count = near_chunks[0]
    first_cut = lax.dynamic_slice(
        random_fields,
        (start, 0, parity("gy") * (rows - HALF), half_of(0) * lanes),
        (count, parts, HALF, lanes),
    )
    own, first_cut = lax.optimization_barrier((random_fields, first_cut))

    cuts = [(0, steps, 1, 0)] + [(s, n, 0, 0) for s, n in near_chunks[1:]]
    cuts += [(s, n, 0, 1) for s, n in far_chunks] + [(0, steps, 1, 1)]
    packed = pl.pallas_call(
        functools.partial(pack_kernel, cuts),
        out_shape=[jax.ShapeDtypeStruct((n, parts, HALF, lanes), kind) for _, n, _, _ in cuts],
        in_specs=[VMEM],
        out_specs=[VMEM] * len(cuts),
        compiler_params=params,
        name="pack",
    )(own)
    near_core = lax.ppermute(packed[0], "gy", core_pairs)
    far_core = lax.ppermute(packed[-1], "gy", core_pairs)
    links = [lax.ppermute(x, "gy", link_pairs) for x in [first_cut, *packed[1:-1]]]
    near_link, far_link = links[: len(near_chunks)], links[len(near_chunks) :]

    depth = cols + HALF * (bool(near_pairs) + bool(far_pairs))
    weights, walls = pl.pallas_call(
        bands_kernel,
        out_shape=(
            jax.ShapeDtypeStruct((rows, rows + 2 * HALF), kind),
            jax.ShapeDtypeStruct((depth, cols), kind),
        ),
        out_specs=(VMEM, VMEM),
        compiler_params=params,
        name="bands",
    )()

    def smooth(start, count, block, core, link):
        return pl.pallas_call(
            functools.partial(smooth_kernel, start, block, 3),
            out_shape=(
                jax.ShapeDtypeStruct((count, parts, rows, lanes), kind),
                jax.ShapeDtypeStruct((count, parts, HALF, rows), kind),
            ),
            in_specs=[VMEM] * 4,
            out_specs=(VMEM, VMEM),
            compiler_params=params,
            cost_estimate=pl.CostEstimate(
                flops=2 * count * parts * rows * lanes * (rows + 2 * HALF),
                bytes_accessed=4 * count * parts * lanes * (rows + HALF),
                transcendentals=0,
            ),
            name="smooth",
        )(weights, own, core, link)

    near = [smooth(s, n, 0, near_core, link) for (s, n), link in zip(near_chunks, near_link)]
    near_halo, far_halo, far = [], [], None
    if near_pairs:
        near_halo = [lax.ppermute(edge, "gz", near_pairs) for _, edge in near]
    if far_pairs:
        far = [smooth(s, n, 1, far_core, link) for (s, n), link in zip(far_chunks, far_link)]
        far_halo = [lax.ppermute(edge, "gz", far_pairs) for _, edge in far]

    hbm = pl.BlockSpec(memory_space=pl.ANY)
    velocity, state, kept = None, previous, None
    for k, (s, n) in enumerate(far_chunks):
        last = k == len(far_chunks) - 1
        used = [q for q, (at, count) in enumerate(near_chunks) if at < s + n and s < at + count]
        operands = [weights, walls, decay, mean_flow, lund_diag, lund_off, state]
        operands += [own if far is None else far[k][0], far_core, far_link[k]]
        operands += [near[q][0] for q in used] + ([near_halo[q] for q in used] if near_halo else []) + far_halo[k : k + 1]
        operands += [out] if k else []
        specs = [VMEM] * len(operands)
        aliases = {}
        if velocity is not None:
            aliases = {len(operands): 0}
            operands.append(velocity)
            specs.append(hbm)
        held = jax.ShapeDtypeStruct((n, parts, rows, cols), jnp.float32)
        shapes, places, scratch = [], [], []
        if kept or last:
            shapes.append(jax.ShapeDtypeStruct((steps, parts, rows, cols), jnp.float32))
            places.append(hbm)
        if last:
            scratch.append(pltpu.VMEM(held.shape, held.dtype))
        else:
            shapes += [jax.ShapeDtypeStruct(previous.shape, jnp.float32), held]
            places += [VMEM, VMEM]
        if kept or last:
            scratch.append(pltpu.SemaphoreType.DMA((bool(kept) + last * n * parts,)))
        made = pl.pallas_call(
            functools.partial(
                velocity_kernel,
                (s, n),
                [near_chunks[q][0] for q in used],
                far is None,
                (bool(near_halo), bool(far_halo)),
                kept,
                last,
            ),
            out_shape=shapes,
            in_specs=specs,
            out_specs=places,
            scratch_shapes=scratch,
            input_output_aliases=aliases,
            compiler_params=params,
            cost_estimate=pl.CostEstimate(
                flops=2 * n * parts * rows * (lanes * (rows + 2 * HALF) + cols * depth),
                bytes_accessed=n * parts * rows * (4 * cols + 10 * lanes),
                transcendentals=0,
            ),
            name="velocity",
        )(*operands)
        velocity = made[0] if kept or last else None
        if not last:
            state, out = made[-2:]
        kept = (s, n)
    return velocity


def solution(mesh):
    return jax.shard_map(
        shards,
        mesh=mesh,
        in_specs=(
            P(None, None, "gy", "gz"),
            P(None, "gy", "gz"),
            P(None, "gz"),
            P(None, "gz"),
            P(None, "gz"),
            P(None, "gz"),
        ),
        out_specs=P(None, None, "gy", "gz"),
        check_vma=False,
    )
```

```python
import functools
import math

import jax
import jax.numpy as jnp
from jax import lax
from jax.experimental import pallas as pl
from jax.experimental.pallas import tpu as pltpu
from jax.sharding import PartitionSpec as P

HALF = 96


VMEM = pl.BlockSpec(memory_space=pltpu.VMEM)
GRANT = 12 * 2**20


def pairs(count, first, closed):
    found = []
    for low in range(first, count, 2):
        if low + 1 < count or closed:
            high = (low + 1) % count
            found += [(low, high), (high, low)]
    return found


def chunks_of(steps):
    cut = lambda ends: [(a, b - a) for a, b in zip([0] + ends, ends)]
    sixteenths = lambda *parts: sorted({max(1, p * steps // 16) for p in parts})
    return cut(sixteenths(5, 11, 16)), cut(sixteenths(5, 10, 13, 15, 16))


def parity(axis):
    return lax.axis_index(axis) % 2


def half_of(block):
    odd = parity("gz")
    return odd if block else 1 - odd


def taps(lag):
    scale = HALF * 1.0
    offsets = lax.broadcasted_iota(jnp.int32, (8, 2 * HALF + 1), 1) - HALF
    offsets = offsets.astype(jnp.float32)
    kernel = jnp.exp(-math.pi * offsets * offsets / (2.0 * scale * scale))
    norm = jnp.sqrt(jnp.sum(kernel * kernel, axis=1, keepdims=True))[:1, :1]
    lag = lag.astype(jnp.float32)
    value = jnp.exp(-math.pi * lag * lag / (2.0 * scale * scale)) / norm
    return jnp.where(jnp.abs(lag) <= HALF, value, jnp.zeros_like(value)).astype(jnp.bfloat16)


def bands_kernel(weights, walls):
    rows = weights.shape[0]
    before, after = -HALF, rows
    odd = parity("gy")
    i = lax.broadcasted_iota(jnp.int32, weights.shape, 0)
    j = lax.broadcasted_iota(jnp.int32, weights.shape, 1)
    at_core = j + jnp.where(odd == 1, before, after)
    at_link = j - HALF - rows + jnp.where(odd == 1, after, before)
    at = jnp.where(j < HALF, at_core, jnp.where(j < HALF + rows, j - HALF, at_link))
    weights[...] = taps(at - i)

    cols = walls.shape[1]
    lanes = cols // 2
    odd = parity("gz")
    j = lax.broadcasted_iota(jnp.int32, walls.shape, 0)
    m = lax.broadcasted_iota(jnp.int32, walls.shape, 1)
    at_far = j + half_of(1) * lanes
    at_near = j - lanes + half_of(0) * lanes
    at_near_halo = j - cols + jnp.where(odd == 1, -HALF, cols)
    at_far_halo = j - cols - HALF + jnp.where(odd == 1, cols, -HALF)
    at = jnp.where(j < cols + HALF, at_near_halo, at_far_halo)
    at = jnp.where(j < lanes, at_far, jnp.where(j < cols, at_near, at))
    walls[...] = taps(at - m)


def pack_kernel(cuts, own, *outs):
    rows = own.shape[2]
    for (start, count, side, block), out in zip(cuts, outs):
        lanes = out.shape[3]
        odd = parity("gy")
        row = pl.multiple_of((1 - odd if side else odd) * (rows - HALF), math.gcd(rows - HALF, 128))
        lane = pl.multiple_of(half_of(block) * lanes, lanes)
        for t in range(count):
            for c in range(own.shape[1]):
                out[t, c] = own[start + t, c, pl.ds(row, HALF), pl.ds(lane, lanes)]


def span_product(weights, core, own, link):
    planes = [jnp.concatenate([core[p], own[p], link[p]], axis=0) for p in range(len(own))]
    return jnp.dot(weights, jnp.concatenate(planes, axis=1), preferred_element_type=jnp.float32)


def smooth_planes(block, start, first, count, weights, own, core, link):
    parts, lanes = own.shape[1], core.shape[3]
    lane = pl.multiple_of(half_of(block) * lanes, lanes)
    index = [(t, c) for t in range(count) for c in range(parts)]
    product = span_product(
        weights[...],
        [core[start + first + t, c] for t, c in index],
        [own[start + first + t, c, :, pl.ds(lane, lanes)] for t, c in index],
        [link[first + t, c] for t, c in index],
    ).astype(own.dtype)
    return {i: product[:, p * lanes : (p + 1) * lanes] for p, i in enumerate(index)}


def smooth_kernel(start, block, per, weights, own, core, link, out, edge):
    steps = out.shape[0]
    width = edge.shape[2]
    for first in range(0, steps, per):
        planes = smooth_planes(block, start, first, min(per, steps - first), weights, own, core, link)
        upper = half_of(block)
        for (t, c), plane in planes.items():
            out[first + t, c] = plane
        turned = {i: plane.T for i, plane in planes.items()}

        @pl.when(upper == 1)
        def _():
            for (t, c), plane in turned.items():
                edge[first + t, c] = plane[plane.shape[0] - width :, :]

        @pl.when(upper == 0)
        def _():
            for (t, c), plane in turned.items():
                edge[first + t, c] = plane[:width, :]


def velocity_kernel(chunk, sources, raw, halos, kept, keeps, last, *refs):
    start, count = chunk
    (weights, walls, decay, mean, diag, off, before, own, core, link), rest = refs[:10], refs[10:]
    near, rest = rest[: len(sources)], rest[len(sources) :]
    near_halo, rest = (rest[: len(sources)], rest[len(sources) :]) if halos[0] else ((), rest)
    far_halo, rest = (rest[:1], rest[1:]) if halos[1] else ((), rest)
    kept_ref, rest = (rest[0], rest[1:]) if kept else (None, rest)
    if keeps:
        state, out = rest[-2:]
    elif last:
        velocity, out, sems = rest[-3:]
    else:
        velocity, state, out, sems = rest[-4:]
    copies = []
    if kept:
        copies.append(pltpu.make_async_copy(kept_ref, velocity.at[pl.ds(*kept)], sems.at[0]))
        copies[0].start()

    parts, rows = own.shape[1:3]
    keep = decay[...]
    fresh = jnp.sqrt(1.0 - keep * keep)
    line = lambda x, c: x[c : c + 1, :]
    u, d, o = mean[...], diag[...], off[...]
    band = walls[...]
    now = [before[c] for c in range(parts)]
    for first in range(0, count, 2):
        group = range(first, min(first + 2, count))
        if raw:
            far = smooth_planes(1, start, first, len(group), weights, own, core, link)
        for t in group:
            step = start + t
            q = max(q for q, at in enumerate(sources) if at <= step)
            cells = []
            for c in range(parts):
                row = [far[t - first, c] if raw else own[t, c], near[q][step - sources[q], c]]
                row += [ref[step - sources[q], c].T for ref in near_halo[q : q + 1]]
                row += [ref[t, c].T for ref in far_halo]
                cells.append(jnp.concatenate(row, axis=1))
            filtered = jnp.dot(jnp.concatenate(cells, axis=0), band, preferred_element_type=jnp.float32)
            for c in range(parts):
                now[c] = line(keep, c) * now[c] + line(fresh, c) * filtered[c * rows : (c + 1) * rows]
                value = line(u, c) + line(d, c) * now[c]
                for e in range(c):
                    value = value + line(o, (c * (c - 1)) // 2 + e) * now[e]
                out[t, c] = value
                if not keeps:
                    k = bool(kept) + t * parts + c
                    copies.append(pltpu.make_async_copy(out.at[t, c], velocity.at[step, c], sems.at[k]))
                    copies[-1].start()
    if not last:
        for c in range(parts):
            state[c] = now[c]
    for copy in copies:
        copy.wait()


def shards(random_fields, previous, decay, mean_flow, lund_diag, lund_off):
    steps, parts, rows, cols = random_fields.shape
    lanes = cols // 2
    span_count = lax.axis_size("gy")
    wall_count = lax.axis_size("gz")
    kind = random_fields.dtype
    params = pltpu.CompilerParams(vmem_limit_bytes=GRANT)

    core_pairs = pairs(span_count, 0, True)
    link_pairs = pairs(span_count, 1, True)
    near_pairs = pairs(wall_count, 0, False)
    far_pairs = pairs(wall_count, 1, False)
    near_chunks, far_chunks = chunks_of(steps)

    start, count = near_chunks[0]
    first_cut = lax.dynamic_slice(
        random_fields,
        (start, 0, parity("gy") * (rows - HALF), half_of(0) * lanes),
        (count, parts, HALF, lanes),
    )
    own, first_cut = lax.optimization_barrier((random_fields, first_cut))

    cuts = [(0, steps, 1, 0)] + [(s, n, 0, 0) for s, n in near_chunks[1:]]
    cuts += [(s, n, 0, 1) for s, n in far_chunks] + [(0, steps, 1, 1)]
    packed = pl.pallas_call(
        functools.partial(pack_kernel, cuts),
        out_shape=[jax.ShapeDtypeStruct((n, parts, HALF, lanes), kind) for _, n, _, _ in cuts],
        in_specs=[VMEM],
        out_specs=[VMEM] * len(cuts),
        compiler_params=params,
        name="pack",
    )(own)
    near_core = lax.ppermute(packed[0], "gy", core_pairs)
    far_core = lax.ppermute(packed[-1], "gy", core_pairs)
    links = [lax.ppermute(x, "gy", link_pairs) for x in [first_cut, *packed[1:-1]]]
    near_link, far_link = links[: len(near_chunks)], links[len(near_chunks) :]

    depth = cols + HALF * (bool(near_pairs) + bool(far_pairs))
    weights, walls = pl.pallas_call(
        bands_kernel,
        out_shape=(
            jax.ShapeDtypeStruct((rows, rows + 2 * HALF), kind),
            jax.ShapeDtypeStruct((depth, cols), kind),
        ),
        out_specs=(VMEM, VMEM),
        compiler_params=params,
        name="bands",
    )()

    def smooth(start, count, block, core, link):
        return pl.pallas_call(
            functools.partial(smooth_kernel, start, block, 2),
            out_shape=(
                jax.ShapeDtypeStruct((count, parts, rows, lanes), kind),
                jax.ShapeDtypeStruct((count, parts, HALF, rows), kind),
            ),
            in_specs=[VMEM] * 4,
            out_specs=(VMEM, VMEM),
            compiler_params=params,
            cost_estimate=pl.CostEstimate(
                flops=2 * count * parts * rows * lanes * (rows + 2 * HALF),
                bytes_accessed=4 * count * parts * lanes * (rows + HALF),
                transcendentals=0,
            ),
            name="smooth",
        )(weights, own, core, link)

    near = [smooth(s, n, 0, near_core, link) for (s, n), link in zip(near_chunks, near_link)]
    near_halo, far_halo, far = [], [], None
    if near_pairs:
        near_halo = [lax.ppermute(edge, "gz", near_pairs) for _, edge in near]
    if far_pairs:
        far = [smooth(s, n, 1, far_core, link) for (s, n), link in zip(far_chunks, far_link)]
        far_halo = [lax.ppermute(edge, "gz", far_pairs) for _, edge in far]

    hbm = pl.BlockSpec(memory_space=pl.ANY)
    velocity, state, kept = None, previous, None
    for k, (s, n) in enumerate(far_chunks):
        last = k == len(far_chunks) - 1
        keeps = k == len(far_chunks) - 2
        used = [q for q, (at, count) in enumerate(near_chunks) if at < s + n and s < at + count]
        operands = [weights, walls, decay, mean_flow, lund_diag, lund_off, state]
        operands += [own if far is None else far[k][0], far_core, far_link[k]]
        operands += [near[q][0] for q in used] + ([near_halo[q] for q in used] if near_halo else []) + far_halo[k : k + 1]
        operands += [out] if kept else []
        specs = [VMEM] * len(operands)
        aliases = {}
        held = jax.ShapeDtypeStruct((n, parts, rows, cols), jnp.float32)
        shapes, places, scratch = [], [], []
        if not keeps:
            if velocity is not None:
                aliases = {len(operands): 0}
                operands.append(velocity)
                specs.append(hbm)
            shapes.append(jax.ShapeDtypeStruct((steps, parts, rows, cols), jnp.float32))
            places.append(hbm)
            scratch.append(pltpu.VMEM(held.shape, held.dtype))
            scratch.append(pltpu.SemaphoreType.DMA((bool(kept) + n * parts,)))
        if not last:
            shapes.append(jax.ShapeDtypeStruct(previous.shape, jnp.float32))
            places.append(VMEM)
        if keeps:
            shapes.append(held)
            places.append(VMEM)
        made = pl.pallas_call(
            functools.partial(
                velocity_kernel,
                (s, n),
                [near_chunks[q][0] for q in used],
                far is None,
                (bool(near_halo), bool(far_halo)),
                kept,
                keeps,
                last,
            ),
            out_shape=shapes,
            in_specs=specs,
            out_specs=places,
            scratch_shapes=scratch,
            input_output_aliases=aliases,
            compiler_params=params,
            cost_estimate=pl.CostEstimate(
                flops=2 * n * parts * rows * (lanes * (rows + 2 * HALF) + cols * depth),
                bytes_accessed=n * parts * rows * (4 * cols + 10 * lanes),
                transcendentals=0,
            ),
            name="velocity",
        )(*operands)
        if keeps:
            state, out = made
        elif last:
            (velocity,) = made
        else:
            velocity, state = made
        kept = (s, n) if keeps else None
    return velocity


def solution(mesh):
    return jax.shard_map(
        shards,
        mesh=mesh,
        in_specs=(
            P(None, None, "gy", "gz"),
            P(None, "gy", "gz"),
            P(None, "gz"),
            P(None, "gz"),
            P(None, "gz"),
            P(None, "gz"),
        ),
        out_specs=P(None, None, "gy", "gz"),
        check_vma=False,
    )
```

```python
import functools
import math

import jax
import jax.numpy as jnp
from jax import lax
from jax.experimental import pallas as pl
from jax.experimental.pallas import tpu as pltpu
from jax.sharding import PartitionSpec as P

HALF = 96


VMEM = pl.BlockSpec(memory_space=pltpu.VMEM)
GRANT = 12 * 2**20


def pairs(count, first, closed):
    found = []
    for low in range(first, count, 2):
        if low + 1 < count or closed:
            high = (low + 1) % count
            found += [(low, high), (high, low)]
    return found


def chunks_of(steps):
    cut = lambda ends: [(a, b - a) for a, b in zip([0] + ends, ends)]
    sixteenths = lambda *parts: sorted({max(1, p * steps // 16) for p in parts})
    return cut(sixteenths(4, 10, 16)), cut(sixteenths(5, 10, 13, 15, 16))


def parity(axis):
    return lax.axis_index(axis) % 2


def half_of(block):
    odd = parity("gz")
    return odd if block else 1 - odd


def taps(lag):
    scale = HALF * 1.0
    offsets = lax.broadcasted_iota(jnp.int32, (8, 2 * HALF + 1), 1) - HALF
    offsets = offsets.astype(jnp.float32)
    kernel = jnp.exp(-math.pi * offsets * offsets / (2.0 * scale * scale))
    norm = jnp.sqrt(jnp.sum(kernel * kernel, axis=1, keepdims=True))[:1, :1]
    lag = lag.astype(jnp.float32)
    value = jnp.exp(-math.pi * lag * lag / (2.0 * scale * scale)) / norm
    return jnp.where(jnp.abs(lag) <= HALF, value, jnp.zeros_like(value)).astype(jnp.bfloat16)


def bands_kernel(weights, walls):
    rows = weights.shape[0]
    before, after = -HALF, rows
    odd = parity("gy")
    i = lax.broadcasted_iota(jnp.int32, weights.shape, 0)
    j = lax.broadcasted_iota(jnp.int32, weights.shape, 1)
    at_core = j + jnp.where(odd == 1, before, after)
    at_link = j - HALF - rows + jnp.where(odd == 1, after, before)
    at = jnp.where(j < HALF, at_core, jnp.where(j < HALF + rows, j - HALF, at_link))
    weights[...] = taps(at - i)

    cols = walls.shape[1]
    lanes = cols // 2
    odd = parity("gz")
    j = lax.broadcasted_iota(jnp.int32, walls.shape, 0)
    m = lax.broadcasted_iota(jnp.int32, walls.shape, 1)
    at_far = j + half_of(1) * lanes
    at_near = j - lanes + half_of(0) * lanes
    at_near_halo = j - cols + jnp.where(odd == 1, -HALF, cols)
    at_far_halo = j - cols - HALF + jnp.where(odd == 1, cols, -HALF)
    at = jnp.where(j < cols + HALF, at_near_halo, at_far_halo)
    at = jnp.where(j < lanes, at_far, jnp.where(j < cols, at_near, at))
    walls[...] = taps(at - m)


def pack_kernel(cuts, own, *outs):
    rows = own.shape[2]
    for (start, count, side, block), out in zip(cuts, outs):
        lanes = out.shape[3]
        odd = parity("gy")
        row = pl.multiple_of((1 - odd if side else odd) * (rows - HALF), math.gcd(rows - HALF, 128))
        lane = pl.multiple_of(half_of(block) * lanes, lanes)
        for t in range(count):
            for c in range(own.shape[1]):
                out[t, c] = own[start + t, c, pl.ds(row, HALF), pl.ds(lane, lanes)]


def span_product(weights, core, own, link):
    planes = [jnp.concatenate([core[p], own[p], link[p]], axis=0) for p in range(len(own))]
    return jnp.dot(weights, jnp.concatenate(planes, axis=1), preferred_element_type=jnp.float32)


def smooth_planes(block, start, first, count, weights, own, core, link):
    parts, lanes = own.shape[1], core.shape[3]
    lane = pl.multiple_of(half_of(block) * lanes, lanes)
    index = [(t, c) for t in range(count) for c in range(parts)]
    product = span_product(
        weights[...],
        [core[start + first + t, c] for t, c in index],
        [own[start + first + t, c, :, pl.ds(lane, lanes)] for t, c in index],
        [link[first + t, c] for t, c in index],
    ).astype(own.dtype)
    return {i: product[:, p * lanes : (p + 1) * lanes] for p, i in enumerate(index)}


def smooth_kernel(start, block, per, weights, own, core, link, out, edge):
    steps = out.shape[0]
    width = edge.shape[2]
    for first in range(0, steps, per):
        planes = smooth_planes(block, start, first, min(per, steps - first), weights, own, core, link)
        upper = half_of(block)
        for (t, c), plane in planes.items():
            out[first + t, c] = plane
        turned = {i: plane.T for i, plane in planes.items()}

        @pl.when(upper == 1)
        def _():
            for (t, c), plane in turned.items():
                edge[first + t, c] = plane[plane.shape[0] - width :, :]

        @pl.when(upper == 0)
        def _():
            for (t, c), plane in turned.items():
                edge[first + t, c] = plane[:width, :]


def velocity_kernel(chunk, sources, raw, halos, kept, keeps, last, *refs):
    start, count = chunk
    (weights, walls, decay, mean, diag, off, before, own, core, link), rest = refs[:10], refs[10:]
    near, rest = rest[: len(sources)], rest[len(sources) :]
    near_halo, rest = (rest[: len(sources)], rest[len(sources) :]) if halos[0] else ((), rest)
    far_halo, rest = (rest[:1], rest[1:]) if halos[1] else ((), rest)
    kept_ref, rest = (rest[0], rest[1:]) if kept else (None, rest)
    if keeps:
        state, out = rest[-2:]
    elif last:
        velocity, out, sems = rest[-3:]
    else:
        velocity, state, out, sems = rest[-4:]
    copies = []
    if kept:
        copies.append(pltpu.make_async_copy(kept_ref, velocity.at[pl.ds(*kept)], sems.at[0]))
        copies[0].start()

    parts, _ = own.shape[1:3]
    keep = decay[...]
    fresh = jnp.sqrt(1.0 - keep * keep)
    line = lambda x, c: x[c : c + 1, :]
    u, d, o = mean[...], diag[...], off[...]
    band = walls[...]
    now = [before[c] for c in range(parts)]
    for first in range(0, count, 2):
        group = range(first, min(first + 2, count))
        if raw:
            far = smooth_planes(1, start, first, len(group), weights, own, core, link)
        for t in group:
            step = start + t
            q = max(q for q, at in enumerate(sources) if at <= step)
            cells = []
            for c in range(parts):
                row = [far[t - first, c] if raw else own[t, c], near[q][step - sources[q], c]]
                row += [ref[step - sources[q], c].T for ref in near_halo[q : q + 1]]
                row += [ref[t, c].T for ref in far_halo]
                cells.append(jnp.concatenate(row, axis=1))
            for c in range(parts):
                filtered = jnp.dot(cells[c], band, preferred_element_type=jnp.float32)
                now[c] = line(keep, c) * now[c] + line(fresh, c) * filtered
                value = line(u, c) + line(d, c) * now[c]
                for e in range(c):
                    value = value + line(o, (c * (c - 1)) // 2 + e) * now[e]
                out[t, c] = value
                if not keeps:
                    k = bool(kept) + t * parts + c
                    copies.append(pltpu.make_async_copy(out.at[t, c], velocity.at[step, c], sems.at[k]))
                    copies[-1].start()
    if not last:
        for c in range(parts):
            state[c] = now[c]
    for copy in copies:
        copy.wait()


def shards(random_fields, previous, decay, mean_flow, lund_diag, lund_off):
    steps, parts, rows, cols = random_fields.shape
    lanes = cols // 2
    span_count = lax.axis_size("gy")
    wall_count = lax.axis_size("gz")
    kind = random_fields.dtype
    params = pltpu.CompilerParams(vmem_limit_bytes=GRANT)
    tight = pltpu.CompilerParams(vmem_limit_bytes=GRANT)

    core_pairs = pairs(span_count, 0, True)
    link_pairs = pairs(span_count, 1, True)
    near_pairs = pairs(wall_count, 0, False)
    far_pairs = pairs(wall_count, 1, False)
    near_chunks, far_chunks = chunks_of(steps)

    start, count = near_chunks[0]
    first_cut = lax.dynamic_slice(
        random_fields,
        (start, 0, parity("gy") * (rows - HALF), half_of(0) * lanes),
        (count, parts, HALF, lanes),
    )
    own, first_cut = lax.optimization_barrier((random_fields, first_cut))

    cuts = [(0, steps, 1, 0)] + [(s, n, 0, 0) for s, n in near_chunks[1:]]
    cuts += [(s, n, 0, 1) for s, n in far_chunks] + [(0, steps, 1, 1)]
    packed = pl.pallas_call(
        functools.partial(pack_kernel, cuts),
        out_shape=[jax.ShapeDtypeStruct((n, parts, HALF, lanes), kind) for _, n, _, _ in cuts],
        in_specs=[VMEM],
        out_specs=[VMEM] * len(cuts),
        compiler_params=params,
        name="pack",
    )(own)
    near_core = lax.ppermute(packed[0], "gy", core_pairs)
    far_core = lax.ppermute(packed[-1], "gy", core_pairs)
    links = [lax.ppermute(x, "gy", link_pairs) for x in [first_cut, *packed[1:-1]]]
    near_link, far_link = links[: len(near_chunks)], links[len(near_chunks) :]

    depth = cols + HALF * (bool(near_pairs) + bool(far_pairs))
    weights, walls = pl.pallas_call(
        bands_kernel,
        out_shape=(
            jax.ShapeDtypeStruct((rows, rows + 2 * HALF), kind),
            jax.ShapeDtypeStruct((depth, cols), kind),
        ),
        out_specs=(VMEM, VMEM),
        compiler_params=params,
        name="bands",
    )()

    def smooth(start, count, block, core, link):
        return pl.pallas_call(
            functools.partial(smooth_kernel, start, block, 2),
            out_shape=(
                jax.ShapeDtypeStruct((count, parts, rows, lanes), kind),
                jax.ShapeDtypeStruct((count, parts, HALF, rows), kind),
            ),
            in_specs=[VMEM] * 4,
            out_specs=(VMEM, VMEM),
            compiler_params=tight,
            cost_estimate=pl.CostEstimate(
                flops=2 * count * parts * rows * lanes * (rows + 2 * HALF),
                bytes_accessed=4 * count * parts * lanes * (rows + HALF),
                transcendentals=0,
            ),
            name="smooth",
        )(weights, own, core, link)

    near = [smooth(s, n, 0, near_core, link) for (s, n), link in zip(near_chunks, near_link)]
    near_halo, far_halo, far = [], [], None
    if near_pairs:
        near_halo = [lax.ppermute(edge, "gz", near_pairs) for _, edge in near]
    if far_pairs:
        far = [smooth(s, n, 1, far_core, link) for (s, n), link in zip(far_chunks, far_link)]
        far_halo = [lax.ppermute(edge, "gz", far_pairs) for _, edge in far]

    hbm = pl.BlockSpec(memory_space=pl.ANY)
    velocity, state, kept = None, previous, None
    for k, (s, n) in enumerate(far_chunks):
        last = k == len(far_chunks) - 1
        keeps = k == len(far_chunks) - 2
        used = [q for q, (at, count) in enumerate(near_chunks) if at < s + n and s < at + count]
        operands = [weights, walls, decay, mean_flow, lund_diag, lund_off, state]
        operands += [own if far is None else far[k][0], far_core, far_link[k]]
        operands += [near[q][0] for q in used] + ([near_halo[q] for q in used] if near_halo else []) + far_halo[k : k + 1]
        operands += [out] if kept else []
        specs = [VMEM] * len(operands)
        aliases = {}
        held = jax.ShapeDtypeStruct((n, parts, rows, cols), jnp.float32)
        shapes, places, scratch = [], [], []
        if not keeps:
            if velocity is not None:
                aliases = {len(operands): 0}
                operands.append(velocity)
                specs.append(hbm)
            shapes.append(jax.ShapeDtypeStruct((steps, parts, rows, cols), jnp.float32))
            places.append(hbm)
            scratch.append(pltpu.VMEM(held.shape, held.dtype))
            scratch.append(pltpu.SemaphoreType.DMA((bool(kept) + n * parts,)))
        if not last:
            shapes.append(jax.ShapeDtypeStruct(previous.shape, jnp.float32))
            places.append(VMEM)
        if keeps:
            shapes.append(held)
            places.append(VMEM)
        made = pl.pallas_call(
            functools.partial(
                velocity_kernel,
                (s, n),
                [near_chunks[q][0] for q in used],
                far is None,
                (bool(near_halo), bool(far_halo)),
                kept,
                keeps,
                last,
            ),
            out_shape=shapes,
            in_specs=specs,
            out_specs=places,
            scratch_shapes=scratch,
            input_output_aliases=aliases,
            compiler_params=tight,
            cost_estimate=pl.CostEstimate(
                flops=2 * n * parts * rows * (lanes * (rows + 2 * HALF) + cols * depth),
                bytes_accessed=n * parts * rows * (4 * cols + 10 * lanes),
                transcendentals=0,
            ),
            name="velocity",
        )(*operands)
        if keeps:
            state, out = made
        elif last:
            (velocity,) = made
        else:
            velocity, state = made
        kept = (s, n) if keeps else None
    return velocity


def solution(mesh):
    return jax.shard_map(
        shards,
        mesh=mesh,
        in_specs=(
            P(None, None, "gy", "gz"),
            P(None, "gy", "gz"),
            P(None, "gz"),
            P(None, "gz"),
            P(None, "gz"),
            P(None, "gz"),
        ),
        out_specs=P(None, None, "gy", "gz"),
        check_vma=False,
    )
```
